32 devices in a mesh: groups: 2 (over y), expert: 8 (over z, x), sub: 2 (over core).
Axes of the slice: x: 2, y: 2, z: 4, core: 2. Of those that a mesh axis runs over, the one named last changes fastest.
Arguments:
- stream_in: bfloat16 [1024, 3072], P(('groups', 'expert'), 'sub'), parts along dimension 0, may hold values from -0.29882812 to 0.29882812
- queries: bfloat16 [1024, 3072], P(('groups', 'expert'), 'sub'), parts along dimension 0, may hold values from -6 to 6
- kv_new: bfloat16 [2, 1024, 1024], P(None, ('groups', 'expert'), 'sub'), parts along dimension 1, may hold values from -6 to 6
- paged_key_value_cache: bfloat16 [2, 32, 4, 1024], P(None, ('groups', 'expert'), None, 'sub'), parts along dimension 1, may hold values from -6 to 6
- page_table: int32 [16, 8], P(('groups', 'expert')), parts along dimension 0, may hold values from 0 to 15, as said below
- prefix_len: int32 [16], P(('groups', 'expert')), parts along dimension 0, may hold values from 8 to 32
- norm_gain: float32 [3072], replicated, may hold values from 0.5 to 1.5
- w_router: bfloat16 [3072, 8], replicated, may hold values from -0.21875 to 0.21875
- expert_ids: int32 [1024, 2], P(('groups', 'expert')), parts along dimension 0, may hold values from 0 to 7, as said below
- w_in: bfloat16 [2, 3072, 65536], P(None, None, ('expert', 'sub')), may hold values from -0.109375 to 0.109375
Outputs:
- stream: bfloat16 [1024, 3072], P(('groups', 'expert'), 'sub'), parts along dimension 0
- expert_hidden: bfloat16 [272, 65536], P('groups', ('expert', 'sub')), parts along dimension 0
The draws below stay inside these ranges and needn't reach their ends.
There are 2 independent parts, one for each index of `groups`. The reference program is written for one: setup_inputs(seed, part) draws one part's arguments, and reference() takes and returns one part's arrays. A program takes and returns all parts, laid end to end along the dimension named above; an argument that names none is the same for every part. Nothing has to cross between parts.
Inputs may be any that keep to these rules, and one draw needn't show every extreme that they name: `expert_ids`: each row names two different experts. The rows of one request name each expert at most 17 times, and one expert is named exactly 17 times by the rows of every request. `page_table`: the pages of one row lie in different shards: page // 2 differs along a row. Requests share leading pages.
All inputs are finite; a program needn't handle non-finite values.
Results may differ from the reference program's by a relative error of at most 0.018.
Values may be sent and summed in bfloat16 or wider, within the bound.
No kernel may reach another device: no remote copies, remote signals or barrier semaphores. Data moves between devices by JAX's collectives and lax.ppermute only.
A program may use at most 128 MiB of HBM per device.

```python
import math
import jax
import jax.numpy as jnp
from jax import lax

D = 3072
QUERY_HEADS = 24
KEY_VALUE_HEADS = 8
HEAD_WIDTH = 128
EXPERTS = 8
FF = 8192
TOP = 2
TOK_DEV = 64
PAGE_TOKENS = 4
CP = 2
REQUEST_COUNT = 8
TABLE_PAGES = 8
CACHE_PAGES = 16
SUFFIX_TOKENS = 512
CAP = 17
GROUP = 1
SLOTS = 136
N_EXPERT = 8


def draw_page_table(key, part):
    family_count = max(REQUEST_COUNT // 4, 1)
    joined_keys = jax.random.split(key, 4)
    family_shift = jax.random.randint(joined_keys[0], (family_count,), 0, TABLE_PAGES)
    shared_len = jax.random.randint(joined_keys[1], (REQUEST_COUNT,), 0, TABLE_PAGES + 1)
    family_pages = jax.random.randint(joined_keys[2], (family_count, TABLE_PAGES), 0, CP)
    own_pages = jax.random.randint(joined_keys[3], (REQUEST_COUNT, TABLE_PAGES), 0, CP)
    family_of = jnp.minimum(jnp.arange(REQUEST_COUNT) // 4, family_count - 1)
    column = jnp.arange(TABLE_PAGES)[None, :]
    inside = jnp.where(column < shared_len[:, None], family_pages[family_of], own_pages)
    owner_dev = (column + family_shift[family_of][:, None]) % TABLE_PAGES
    return (owner_dev * CP + inside).astype(jnp.int32)


def draw_prefix_len(key, part):
    joined_keys = jax.random.split(key, 2)
    lengths = jax.random.randint(joined_keys[0], (REQUEST_COUNT,), PAGE_TOKENS * TABLE_PAGES // 4, PAGE_TOKENS * TABLE_PAGES + 1)
    longest = jax.random.randint(joined_keys[1], (), 0, REQUEST_COUNT)
    return jnp.where(jnp.arange(REQUEST_COUNT) == longest, PAGE_TOKENS * TABLE_PAGES, lengths).astype(jnp.int32)


def draw_queries(key, part):
    root_random_key = jax.random.fold_in(key, 11)
    value_rows = jnp.clip(jax.random.normal(root_random_key, (SUFFIX_TOKENS, QUERY_HEADS * HEAD_WIDTH), jnp.float32), -6.0, 6.0)
    return value_rows.astype(jnp.bfloat16)


def draw_kv_new(key, part):
    root_random_key = jax.random.fold_in(key, 13)
    value_rows = jnp.clip(jax.random.normal(root_random_key, (2, SUFFIX_TOKENS, KEY_VALUE_HEADS * HEAD_WIDTH), jnp.float32), -6.0, 6.0)
    return value_rows.astype(jnp.bfloat16)


def shuffled(one_key):
    return jax.random.permutation(one_key, TOK_DEV)


def unit_order(one_key):
    return jax.random.permutation(one_key, (EXPERTS - 1) * CAP)


def draw_expert_ids(key, part):
    joined_keys = jax.random.split(jax.random.fold_in(key, 17), 4)
    hot_expert = jax.random.randint(joined_keys[0], (), 0, EXPERTS)
    remaining = TOK_DEV * TOP - CAP
    units = jax.vmap(unit_order)(jax.random.split(joined_keys[1], REQUEST_COUNT))
    picked = units[:, :remaining] // CAP
    other_counts = jnp.sum((picked[:, :, None] == jnp.arange(EXPERTS - 1)[None, None, :]).astype(jnp.int32), axis=1)
    expert_range = jnp.arange(EXPERTS)
    offset = (expert_range - hot_expert - 1) % EXPERTS
    counts = jnp.where(expert_range[None, :] == hot_expert, CAP, jnp.take(other_counts, jnp.minimum(offset, EXPERTS - 2), axis=1))
    route_ends = jnp.cumsum(counts, axis=1)
    route_pos = jnp.arange(TOK_DEV * TOP)
    sequence = jnp.sum((route_pos[None, :, None] >= route_ends[:, None, :]).astype(jnp.int32), axis=2)
    pair_ids = jnp.stack([sequence[:, :TOK_DEV], sequence[:, TOK_DEV:]], axis=2)
    flip_bits = jax.random.randint(joined_keys[2], (REQUEST_COUNT, TOK_DEV, 1), 0, 2)
    pair_ids = jnp.where(flip_bits == 1, pair_ids[:, :, ::-1], pair_ids)
    orders = jax.vmap(shuffled)(jax.random.split(joined_keys[3], REQUEST_COUNT))
    pair_ids = jnp.take_along_axis(pair_ids, orders[:, :, None], axis=1)
    return pair_ids.reshape(SUFFIX_TOKENS, TOP).astype(jnp.int32)


def levels(stream_key, extent, cuts, least, top_value):
    def one(dim, blocks):
        steps = jax.random.uniform(jax.random.fold_in(jax.random.fold_in(stream_key, 6), dim), (blocks,), jnp.float32, least / len(cuts), top_value / len(cuts))
        return jnp.repeat(jnp.exp(steps), extent[dim] // blocks).reshape((-1,) + (1,) * (len(extent) - dim - 1))

    loudness = one(*cuts[0])
    for cut in cuts[1:]:
        loudness = loudness * one(*cut)
    return loudness


def bell_draw(stream_key, shape, deviation, reach, pieces=(), kind=jnp.bfloat16):
    result = jax.random.normal(stream_key, shape, jnp.float32) * deviation
    if len(pieces) > 0:
        result = levels(stream_key, shape, pieces, -0.22, 0.18) * result
    return jnp.clip(result, min=-reach, max=reach).astype(kind)


def setup_inputs(seed: int = 0, part: int = 0) -> dict:
    splits = jax.random.split(jax.random.key(seed), 11)
    part_keys = jax.random.split(jax.random.fold_in(splits[10], part), 11)
    return {
        "stream_in": bell_draw(part_keys[0], (SUFFIX_TOKENS, D), 0.05, 0.29882812, ((0, 8), (1, 2))),
        "queries": draw_queries(jax.random.fold_in(jax.random.fold_in(splits[10], part), 71), part),
        "kv_new": draw_kv_new(jax.random.fold_in(jax.random.fold_in(splits[10], part), 71), part),
        "paged_key_value_cache": bell_draw(part_keys[3], (2, CACHE_PAGES, PAGE_TOKENS, KEY_VALUE_HEADS * HEAD_WIDTH), 1.0, 6.0, ((1, 8), (3, 2))),
        "page_table": draw_page_table(jax.random.fold_in(jax.random.fold_in(splits[10], part), 71), part),
        "prefix_len": draw_prefix_len(jax.random.fold_in(jax.random.fold_in(splits[10], part), 71), part),
        "norm_gain": jnp.clip(1.0 + 0.1 * jax.random.normal(splits[6], (D,), jnp.float32), 0.5, 1.5),
        "w_router": bell_draw(splits[7], (D, EXPERTS), (D // 4) ** -0.5, 0.21875),
        "expert_ids": draw_expert_ids(jax.random.fold_in(jax.random.fold_in(splits[10], part), 71), part),
        "w_in": bell_draw(splits[9], (2, D, EXPERTS * FF), D ** -0.5, 0.109375, ((2, 16),)),
    }


def attend(query_rows, key_rows, prefix_length, head_size):
    tokens_here = query_rows.shape[0]
    length = key_rows.shape[1]
    kv_heads = key_rows.shape[2] // head_size
    grouped = query_rows.shape[1] // head_size // kv_heads
    query_f = query_rows.reshape(tokens_here, kv_heads, grouped, head_size).astype(jnp.float32)
    keys_f = key_rows[0].reshape(length, kv_heads, head_size).astype(jnp.float32)
    values_f = key_rows[1].reshape(length, kv_heads, head_size).astype(jnp.float32)
    scores = jnp.einsum('tkgd,lkd->kgtl', query_f, keys_f) * (1.0 / math.sqrt(head_size))
    prefix_span = length - tokens_here
    places = jnp.arange(length)[None, :]
    rows_at = jnp.arange(tokens_here)[:, None]
    is_live = jnp.where(places < prefix_span, places < prefix_length, places - prefix_span <= rows_at)
    scores = jnp.where(is_live, scores, -1e+30)
    largest = lax.optimization_barrier(jnp.max(scores, axis=-1, keepdims=True))
    exponent = jnp.exp(scores - largest)
    weights = (exponent / lax.optimization_barrier(jnp.sum(exponent, axis=-1, keepdims=True))).astype(jnp.bfloat16)
    mixed_heads = jnp.einsum('kgtl,lkd->tkgd', weights.astype(jnp.float32), values_f)
    return mixed_heads.reshape(tokens_here, -1).astype(jnp.bfloat16)

def reference(stream_in, queries, kv_new, paged_key_value_cache, page_table, prefix_len, norm_gain, w_router, expert_ids, w_in):

    def one_request(request):
        page_list = page_table[request]
        page_row_block = jnp.take(paged_key_value_cache, page_list, axis=1)
        prefix_row_block = page_row_block.reshape(2, TABLE_PAGES * PAGE_TOKENS, KEY_VALUE_HEADS * HEAD_WIDTH)
        row_start = (request * TOK_DEV).astype(jnp.int32)
        suffix = lax.dynamic_slice_in_dim(kv_new, row_start, TOK_DEV, 1)
        query_rows = lax.dynamic_slice_in_dim(queries, row_start, TOK_DEV, 0)
        key_rows = jnp.concatenate([prefix_row_block, suffix], axis=1)
        return attend(query_rows, key_rows, prefix_len[request], HEAD_WIDTH)
    attended = lax.map(one_request, jnp.arange(REQUEST_COUNT, dtype=jnp.int32)).reshape(SUFFIX_TOKENS, QUERY_HEADS * HEAD_WIDTH)
    stream = (stream_in.astype(jnp.float32) + attended.astype(jnp.float32)).astype(jnp.bfloat16)
    stream_f = stream.astype(jnp.float32)
    scale_rows = lax.rsqrt(lax.optimization_barrier(jnp.mean(stream_f * stream_f, axis=-1, keepdims=True)) + 1e-05)
    normed = (stream_f * scale_rows * norm_gain).astype(jnp.bfloat16)
    logits = jnp.dot(normed, w_router, preferred_element_type=jnp.float32)
    chosen = jnp.take_along_axis(logits, expert_ids, axis=1)
    gate_share = jax.nn.sigmoid(chosen - chosen[:, ::-1])
    route_ids = expert_ids.reshape(N_EXPERT, TOK_DEV * TOP)
    expert_hot = (route_ids[:, :, None] == jnp.arange(EXPERTS, dtype=jnp.int32)[None, None, :]).astype(jnp.int32)
    route_rank = lax.optimization_barrier(jnp.sum((jnp.cumsum(expert_hot, axis=1) - 1) * expert_hot, axis=2)).astype(jnp.int32)
    request_ids = jnp.arange(N_EXPERT, dtype=jnp.int32)
    slot_base = ((request_ids % GROUP * EXPERTS + request_ids // GROUP) * CAP).astype(jnp.int32)
    slot_at = (slot_base[:, None] + route_rank).astype(jnp.int32)
    token_at = (request_ids[:, None] * TOK_DEV + jnp.arange(TOK_DEV * TOP, dtype=jnp.int32)[None, :] // TOP).astype(jnp.int32)
    token_slots = jnp.zeros((EXPERTS, SLOTS), jnp.int32).at[route_ids, slot_at].set(token_at)
    share_flat = gate_share.reshape(N_EXPERT, TOK_DEV * TOP)
    slot_shares = jnp.zeros((EXPERTS, SLOTS), jnp.float32).at[route_ids, slot_at].set(share_flat)
    columns = []
    for expert in range(EXPERTS):
        slot_rows = jnp.take(normed, token_slots[expert], axis=0)
        gate_part = jnp.dot(slot_rows, w_in[0, :, expert * FF:(expert + 1) * FF], preferred_element_type=jnp.float32)
        up_part = jnp.dot(slot_rows, w_in[1, :, expert * FF:(expert + 1) * FF], preferred_element_type=jnp.float32)
        columns.append((jax.nn.silu(gate_part) * up_part * slot_shares[expert][:, None]).astype(jnp.bfloat16))
    return (stream, jnp.concatenate(columns, axis=1))
```

```python
import math

import jax
import jax.numpy as jnp
from jax import lax
from jax.experimental import pallas as pl
from jax.experimental.pallas import tpu as pltpu
from jax.sharding import PartitionSpec as P

HEAD_WIDTH = 128
EXPERTS = 8
TOP = 2
CAP = 17
LANES = 128
MIB = 1 << 20
FIRST = (0, 3)
BF16 = jnp.bfloat16
F32 = jnp.float32


def swap(array, axis, bit):
    return lax.ppermute(array, axis, [(i, i ^ (1 << bit)) for i in range(lax.axis_size(axis))])


def from_behind(array, axis, steps):
    count = lax.axis_size(axis)
    return lax.ppermute(array, axis, [(i, (i + steps) % count) for i in range(count)])


def mm(a, b):
    return jnp.dot(a, b, preferred_element_type=F32)


def mm_t(a, b):
    return lax.dot_general(a, b, (((1,), (1,)), ((), ())), preferred_element_type=F32)


def attend_kernel(q_ref, new_ref, pages_ref, hot_ref, plen_ref, in_ref, pick_ref, noted_ref,
                  stream_ref, out_refs):
    tokens = q_ref.shape[0]
    kv_heads = new_ref.shape[2] // HEAD_WIDTH
    grouped = q_ref.shape[1] // HEAD_WIDTH // kv_heads
    prefix = hot_ref.shape[0]
    pages = pages_ref[...].astype(F32)
    width = new_ref.shape[2]
    hot = hot_ref[...]
    keys_p = mm(hot, pages[:, 0].reshape(-1, width).astype(BF16)).astype(BF16)
    vals_p = mm(hot, pages[:, 1].reshape(-1, width).astype(BF16)).astype(BF16)
    rows = grouped * tokens
    live_p = lax.broadcasted_iota(jnp.int32, (rows, prefix), 1) < plen_ref[0]
    at = lax.broadcasted_iota(jnp.int32, (rows, tokens), 0) % tokens
    live_n = lax.broadcasted_iota(jnp.int32, (rows, tokens), 1) <= at
    factor = 1.0 / math.sqrt(HEAD_WIDTH)
    for k in range(kv_heads):
        cols = pl.ds(k * HEAD_WIDTH, HEAD_WIDTH)
        sl = slice(k * HEAD_WIDTH, (k + 1) * HEAD_WIDTH)
        heads = [k * grouped + g for g in range(grouped)]
        q = jnp.concatenate(
            [q_ref[:, h * HEAD_WIDTH : (h + 1) * HEAD_WIDTH] for h in heads], axis=0
        )
        s_p = jnp.where(live_p, mm_t(q, keys_p[:, sl]) * factor, -1e30)
        s_n = jnp.where(live_n, mm_t(q, new_ref[0, :, cols]) * factor, -1e30)
        top = jnp.maximum(
            jnp.max(s_p, axis=-1, keepdims=True), jnp.max(s_n, axis=-1, keepdims=True)
        )
        e_p = jnp.exp(s_p - top)
        e_n = jnp.exp(s_n - top)
        total = jnp.sum(e_p, axis=-1, keepdims=True) + jnp.sum(e_n, axis=-1, keepdims=True)
        w_p = (e_p / total).astype(BF16)
        w_n = (e_n / total).astype(BF16)
        mixed = (mm(w_p, vals_p[:, sl]) + mm(w_n, new_ref[1, :, cols])).astype(BF16)
        for g, h in enumerate(heads):
            hs = slice(h * HEAD_WIDTH, (h + 1) * HEAD_WIDTH)
            part = mixed[g * tokens : (g + 1) * tokens].astype(F32)
            stream_ref[:, hs] = (in_ref[:, hs].astype(F32) + part).astype(BF16)
    sent = mm(pick_ref[...], stream_ref[...])
    width = stream_ref.shape[1]
    padded = sent.shape[0] // EXPERTS
    folds = width // LANES
    spare = CAP - 1 - folds - 1
    for e, out_ref in enumerate(out_refs):
        first = e * padded
        out_ref[:, :width] = sent[first : first + CAP - 1].astype(BF16)
        last = sent[first + CAP - 1 : first + CAP]
        lines = [last[:, c * LANES : (c + 1) * LANES] for c in range(folds)]
        lines += [noted_ref[e : e + 1, :], jnp.zeros((spare, LANES), F32)]
        out_ref[:, width:] = jnp.concatenate(lines, axis=0).astype(BF16)


def attend(queries, kv_new, pages, hot, prefix_len, stream_in, pick, noted, marks):
    tokens, width = stream_in.shape
    vm = pl.BlockSpec(memory_space=pltpu.VMEM)

    def body(*refs):
        inputs = refs[:8]
        outputs = refs[8 + len(marks) :]
        attend_kernel(*inputs, outputs[0], outputs[1:])

    return pl.pallas_call(
        body,
        out_shape=[jax.ShapeDtypeStruct((tokens, width), BF16)]
        + [jax.ShapeDtypeStruct((CAP - 1, width + LANES), BF16)] * EXPERTS,
        in_specs=[vm, vm, vm, vm, pl.BlockSpec(memory_space=pltpu.SMEM), vm, vm, vm]
        + [vm] * len(marks),
        out_specs=[vm] * (1 + EXPERTS),
        compiler_params=pltpu.CompilerParams(vmem_limit_bytes=8 * MIB),
        name="attend",
    )(queries, kv_new, pages, hot, prefix_len, stream_in, pick, noted, *marks)


def assemble(parts, marks, group_width):
    width = parts[0].shape[1] - LANES
    slots = EXPERTS * CAP
    padded = -(-CAP // 8) * 8

    def body(*refs):
        home = lax.axis_index("expert") // group_width
        rows_ref, code_ref = refs[EXPERTS + len(marks) :]
        stacked, codes = [], []
        for ref in refs[:EXPERTS]:
            extra = ref[:, width:].astype(F32)
            stacked.append(ref[:, :width].astype(F32))
            lines = [extra[c : c + 1] for c in range(width // LANES)]
            stacked.append(jnp.concatenate(lines, axis=1))
            stacked.append(jnp.zeros((padded - CAP, width), F32))
            codes.append(extra[width // LANES : width // LANES + 1])
        whole = jnp.concatenate(stacked, axis=0).astype(BF16)
        slot = lax.broadcasted_iota(jnp.int32, (slots, padded * EXPERTS), 0)
        column = lax.broadcasted_iota(jnp.int32, (slots, padded * EXPERTS), 1)
        stride = (home - slot // CAP + EXPERTS) % EXPERTS
        order = (column == stride * padded + slot % CAP).astype(F32).astype(BF16)
        rows_ref[...] = mm(order, whole).astype(BF16)
        slot = lax.broadcasted_iota(jnp.int32, (slots, LANES), 0)
        lane = lax.broadcasted_iota(jnp.int32, (slots, LANES), 1)
        stride = (home - slot // CAP + EXPERTS) % EXPERTS
        code = jnp.zeros((slots, 1), F32)
        for k in range(EXPERTS):
            wanted = (lane == slot % CAP) & (stride == k)
            code += jnp.sum(jnp.where(wanted, codes[k], 0.0), axis=1, keepdims=True)
        code_ref[...] = jnp.broadcast_to(code, (slots, LANES)).astype(BF16)

    vm = pl.BlockSpec(memory_space=pltpu.VMEM)
    return pl.pallas_call(
        body,
        out_shape=(
            jax.ShapeDtypeStruct((slots, width), BF16),
            jax.ShapeDtypeStruct((slots, LANES), BF16),
        ),
        in_specs=[vm] * (EXPERTS + len(marks)),
        out_specs=(vm, vm),
        compiler_params=pltpu.CompilerParams(vmem_limit_bytes=8 * MIB),
        name="assemble",
    )(*parts, *marks)


def preload(w_in, first, count, after, name):
    depth = w_in.shape[1]

    def body(w_ref, *refs):
        o_ref, done_ref, sem = refs[len(after) :]
        copy = pltpu.make_async_copy(w_ref.at[:, :, pl.ds(first, count)], o_ref, sem)
        copy.start()
        done_ref[...] = jnp.zeros_like(done_ref)
        copy.wait()

    anywhere = pl.BlockSpec(memory_space=pl.ANY)
    return pl.pallas_call(
        body,
        out_shape=(
            pltpu.VMEM((2, depth, count), BF16),
            jax.ShapeDtypeStruct((8, LANES), F32),
        ),
        in_specs=[anywhere] * (1 + len(after)),
        out_specs=(pl.BlockSpec(memory_space=pltpu.VMEM), pl.BlockSpec(memory_space=pltpu.VMEM)),
        scratch_shapes=[pltpu.SemaphoreType.DMA],
        compiler_params=pltpu.CompilerParams(vmem_limit_bytes=MIB),
        cost_estimate=pl.CostEstimate(
            flops=0, transcendentals=0, bytes_accessed=4 * depth * count
        ),
        name=name,
    )(w_in, *after)


def experts(own, other, code, group_width, gain, router, w_in, held):
    slots = own.shape[0]
    half = own.shape[1]
    depth = 2 * half
    columns = w_in.shape[2]
    held_columns = [h.shape[2] for h in held]
    rest = columns - sum(held_columns)
    start_rest = sum(held_columns)
    block = next(b for b in (256, 128) if all(c % b == 0 for c in [rest] + held_columns))
    pieces = rest // block
    ring = min(pieces, 3)

    def body(*refs):
        own_ref, other_ref, code_ref, gain_ref, router_ref, w_ref = refs[:6]
        held_refs = refs[6 : 6 + len(held)]
        out_ref, rest_ref, normed_ref, sems = refs[6 + len(held) :]

        def fetch(i):
            return pltpu.make_async_copy(
                w_ref.at[:, :, pl.ds(start_rest + i * block, block)],
                rest_ref.at[i % ring],
                sems.at[i % ring],
            )

        for i in range(ring):
            fetch(i).start()
        first = lax.axis_index("sub") == 0
        mine = own_ref[...]
        theirs = other_ref[...]
        low = jnp.where(first, mine, theirs).astype(F32)
        high = jnp.where(first, theirs, mine).astype(F32)
        square = jnp.sum(low * low, axis=1, keepdims=True) + jnp.sum(
            high * high, axis=1, keepdims=True
        )
        scale = lax.rsqrt(square * (1.0 / depth) + 1e-05)
        normed_ref[:, :half] = (low * scale * gain_ref[:, :half]).astype(BF16)
        normed_ref[:, half:] = (high * scale * gain_ref[:, half:]).astype(BF16)
        logits = mm_t(normed_ref[...], router_ref[...])
        here = lax.axis_index("expert") // group_width
        code = code_ref[...].astype(F32)[:, :1].astype(jnp.int32)
        away = code - 1 - here
        lane = lax.broadcasted_iota(jnp.int32, logits.shape, 1)
        mine_logit = jnp.sum(jnp.where(lane == here, logits, 0.0), axis=1, keepdims=True)
        away_logit = jnp.sum(jnp.where(lane == away, logits, 0.0), axis=1, keepdims=True)
        share = 1.0 / (1.0 + jnp.exp(away_logit - mine_logit))
        share = jnp.where(code > 0, share, 0.0)

        def hidden(gate_w, up_w):
            rows = normed_ref[...]
            gate = mm(rows, gate_w)
            up = mm(rows, up_w)
            return (gate / (1.0 + jnp.exp(-gate)) * up * share).astype(BF16)

        def rest_block(i):
            fetch(i).wait()
            at = start_rest + i * block
            out_ref[:, at : at + block] = hidden(rest_ref[i % ring, 0], rest_ref[i % ring, 1])
            if i + ring < pieces:
                fetch(i + ring).start()

        kept = [
            (h_ref, i)
            for h_ref, count in zip(held_refs, held_columns)
            for i in range(count // block)
        ]
        spacing = max(len(kept) // pieces, 1)
        done = 0
        for n in range(len(kept)):
            h_ref, i = kept[n]
            at = slice(i * block, (i + 1) * block)
            out_ref[:, n * block : (n + 1) * block] = hidden(h_ref[0, :, at], h_ref[1, :, at])
            if (n + 1) % spacing == 0 and done < pieces:
                rest_block(done)
                done += 1
        for i in range(done, pieces):
            rest_block(i)

    vm = pl.BlockSpec(memory_space=pltpu.VMEM)
    return pl.pallas_call(
        body,
        out_shape=jax.ShapeDtypeStruct((slots, columns), BF16),
        in_specs=[vm, vm, vm, vm, vm,
                  pl.BlockSpec(memory_space=pl.ANY)] + [vm] * len(held),
        out_specs=vm,
        scratch_shapes=[
            pltpu.VMEM((ring, 2, depth, block), BF16),
            pltpu.VMEM((slots, depth), BF16),
            pltpu.SemaphoreType.DMA((ring,)),
        ],
        compiler_params=pltpu.CompilerParams(
            vmem_limit_bytes=(60 if not held else 17) * MIB
        ),
        name="experts",
    )(own, other, code, gain, router, w_in, *held)


def shards(stream_in, queries, kv_new, paged_key_value_cache, page_table, prefix_len, norm_gain,
           w_router, expert_ids, w_in):
    expert_count = lax.axis_size("expert")
    group_width = expert_count // EXPERTS
    level_values = group_width.bit_length() - 1
    own_index = lax.axis_index("expert")
    own_group = own_index // group_width
    tokens, half = stream_in.shape
    cache = paged_key_value_cache
    page_rows = cache.shape[2]
    shard_rows = cache.shape[1] * page_rows
    columns = w_in.shape[2]
    step = columns // 8 // LANES * LANES

    mine = cache.reshape(1, 2, shard_rows, cache.shape[3])
    pages = lax.all_to_all(
        jnp.broadcast_to(mine, (expert_count,) + mine.shape[1:]), "expert", 0, 0, tiled=True
    )
    early, late = FIRST
    held, marks = [], []
    wanted = (
        page_table[0][:, None] * page_rows + jnp.arange(page_rows, dtype=jnp.int32)[None, :]
    ).reshape(-1, 1)
    hot = (
        wanted == jnp.arange(expert_count * shard_rows, dtype=jnp.int32)[None, :]
    ).astype(BF16)

    named = jnp.sum(
        (expert_ids[:, :, None] == jnp.arange(EXPERTS, dtype=jnp.int32)).astype(jnp.int32), axis=1
    )
    rank = jnp.cumsum(named, axis=0) - named
    slot = jnp.where(named > 0, rank, -1).T
    towards = (own_group + jnp.arange(EXPERTS, dtype=jnp.int32)) % EXPERTS
    slot = jnp.take(slot, towards, axis=0)
    padded = -(-CAP // 16) * 16
    pick = (
        (slot[:, None, :] == jnp.arange(padded, dtype=jnp.int32)[None, :, None])
        .astype(BF16)
        .reshape(EXPERTS * padded, tokens)
    )
    total = jnp.sum(expert_ids, axis=1) + 1
    chosen = slot[:, None, :] == jnp.arange(LANES, dtype=jnp.int32)[None, :, None]
    noted = jnp.sum(jnp.where(chosen, total[None, None, :], 0), axis=2).astype(F32)
    if step >= 256 and early:
        kept, mark = preload(w_in, 0, early * step, (hot, pick, noted), "preload_first")
        held.append(kept)
        marks.append(mark)
    stream, *outgoing = attend(
        queries, kv_new, pages, hot, prefix_len, stream_in, pick, noted, marks
    )
    parts = [outgoing[0]] + [
        from_behind(outgoing[k], "expert", k * group_width) for k in range(1, EXPERTS)
    ]
    marks = []
    if step >= 256 and late:
        kept, mark = preload(w_in, early * step, late * step, outgoing[:1], "preload_second")
        held.append(kept)
        marks.append(mark)
    rows, code = assemble(parts, marks, group_width)
    rows, code = rows[None], code[None]
    for bit in range(level_values):
        is_high = (own_index >> bit) % 2 == 1
        rows, code = (
            jnp.concatenate(
                [jnp.where(is_high, there, here), jnp.where(is_high, here, there)], axis=0
            )
            for here, there in ((rows, swap(rows, "expert", bit)), (code, swap(code, "expert", bit)))
        )
    rows = rows.reshape(-1, half)
    code = code.reshape(-1, LANES)
    other = swap(rows, "sub", 0)
    hidden = experts(
        rows, other, code, group_width, norm_gain[None, :], w_router.T, w_in, held
    )
    return (stream, hidden)


def solution(mesh):
    placed = (
        P(("groups", "expert"), "sub"),
        P(("groups", "expert"), "sub"),
        P(None, ("groups", "expert"), "sub"),
        P(None, ("groups", "expert"), None, "sub"),
        P(("groups", "expert"), None),
        P(("groups", "expert")),
        P(),
        P(),
        P(("groups", "expert"), None),
        P(None, None, ("expert", "sub")),
    )
    return jax.shard_map(
        shards,
        mesh=mesh,
        in_specs=placed,
        out_specs=(P(("groups", "expert"), "sub"), P("groups", ("expert", "sub"))),
        check_vma=False,
    )
```
